32 devices in a mesh: batch: 4 (over z), seq: 4 (over y, core), head: 2 (over x).
Axes of the slice: x: 2, y: 2, z: 4, core: 2. Of those that a mesh axis runs over, the one named last changes fastest.
Arguments:
- image_hidden: bfloat16 [8, 1024, 3072], P('batch', 'seq', 'head'), parts along dimension 0, may hold values from -6 to 6
- modulation: float32 [8, 3, 3072], P('batch'), parts along dimension 0, may hold values from -4 to 4
- qkv_weight: bfloat16 [3072, 3, 1536], P(None, None, 'head'), may hold values from -0.109375 to 0.109375
- out_weight: bfloat16 [1536, 3072], P('head'), may hold values from -0.15625 to 0.15625
- q_gain: float32 [128], replicated, may hold values from 1.2 to 2.5
- k_gain: float32 [128], replicated, may hold values from 1.2 to 2.5
- text_keys: bfloat16 [8, 128, 1536], P('batch', 'seq', 'head'), parts along dimension 0, may hold values from -10 to 10
- text_values: bfloat16 [8, 128, 1536], P('batch', 'seq', 'head'), parts along dimension 0, may hold values from -6 to 6
- stale_keys: bfloat16 [8, 1024, 1536], P('batch', 'seq', 'head'), parts along dimension 0, may hold values from -64 to 64
- stale_values: bfloat16 [8, 1024, 1536], P('batch', 'seq', 'head'), parts along dimension 0, may hold values from -6 to 6
- cached_residual: bfloat16 [8, 1024, 3072], P('batch', 'seq', 'head'), parts along dimension 0, may hold values from -6 to 6
- patch_of: int32 [16], P('batch'), parts along dimension 0, may hold values from 0 to 3, each once
- refresh: int32 [16], P('batch'), parts along dimension 0, may hold values from 0 to 1, as said below
- text_len: int32 [8], P('batch'), parts along dimension 0, may hold values from 16 to 128
Outputs:
- image_out: bfloat16 [8, 1024, 3072], P('batch', 'seq', 'head'), parts along dimension 0
The draws below stay inside these ranges and needn't reach their ends.
There are 4 independent parts, one for each index of `batch`. The reference program is written for one: setup_inputs(seed, part) draws one part's arguments, and reference() takes and returns one part's arrays. A program takes and returns all parts, laid end to end along the dimension named above; an argument that names none is the same for every part. Nothing has to cross between parts.
Inputs may be any that keep to these rules, and one draw needn't show every extreme that they name: `patch_of`: A permutation: every image band sits on exactly one index of seq. `refresh`: exactly 1 entries are 1, the rest 0.
All inputs are finite; a program needn't handle non-finite values.
Results may differ from the reference program's by a relative error of at most 0.012.
The reference program's roundings to bfloat16 on the way count: a program that leaves them out, or rounds other values in their place, can miss the bound.
Values may be sent and summed in bfloat16 or wider, within the bound.
A program may use at most 192 MiB of HBM per device.

```python
import math
import jax
import jax.numpy as jnp
from jax import lax

D = 3072
HEADS = 12
HEAD_DIM = 128
GRID_W = 64
PROMPTS = 2
IMG_DEV = 256
IMG = 1024
TXT = 128
REFRESH = 1
N_SEQ = 4


def draw_stale_keys(key, part):
    shape = (PROMPTS, IMG, HEADS * HEAD_DIM)
    drawn = 1.8 * jax.random.truncated_normal(key, -5.0, 5.0, shape, jnp.float32)
    return drawn.astype(jnp.bfloat16)


def draw_refresh(key, part):
    shuffled = jax.random.permutation(key, N_SEQ)
    return (shuffled < REFRESH).astype(jnp.int32)


def steps_of(rng, shape, cuts, low, top_value):
    factor_of, own = 1.0, jax.random.fold_in(rng, 6)
    for dim, parts in cuts:
        heights = jnp.exp(jax.random.uniform(jax.random.fold_in(own, dim), (parts,), jnp.float32, low / len(cuts), top_value / len(cuts)))
        factor_of = factor_of * jnp.repeat(heights, shape[dim] // parts).reshape([-1 if axis == dim else 1 for axis in range(len(shape))])
    return factor_of


def bell_draw(own_key, extent, spread, limit, cuts=(), kind=jnp.bfloat16):
    level = steps_of(own_key, extent, cuts, -0.22, 0.18) if cuts else 1.0
    entries = jax.random.normal(own_key, extent, jnp.float32) * spread * level
    return jnp.minimum(jnp.maximum(entries, -limit), limit).astype(kind)


def setup_inputs(seed: int = 0, part: int = 0) -> dict:
    key_list = jax.random.split(jax.random.key(seed), 15)
    part_keys = jax.random.split(jax.random.fold_in(key_list[14], part), 15)
    image_hidden = bell_draw(part_keys[0], (PROMPTS, IMG, D), 1.0, 6.0, ((1, 4), (2, 2)))
    modulation = bell_draw(part_keys[1], (PROMPTS, 3, D), 0.8, 4.0, (), jnp.float32)
    qkv_weight = bell_draw(key_list[2], (D, 3, HEADS * HEAD_DIM), D ** -0.5, 0.109375, ((2, 2),))
    out_weight = bell_draw(key_list[3], (HEADS * HEAD_DIM, D), (HEADS * HEAD_DIM) ** -0.5, 0.15625, ((0, 2),))
    q_gain = jnp.clip(jnp.exp(jax.random.uniform(key_list[4], (HEAD_DIM,), jnp.float32, math.log(1.2), math.log(2.5))), 1.2, 2.5)
    k_gain = jnp.clip(jnp.exp(jax.random.uniform(key_list[5], (HEAD_DIM,), jnp.float32, math.log(1.2), math.log(2.5))), 1.2, 2.5)
    text_keys = bell_draw(part_keys[6], (PROMPTS, TXT, HEADS * HEAD_DIM), 1.8, 10.0, ((1, 4), (2, 2)))
    text_values = bell_draw(part_keys[7], (PROMPTS, TXT, HEADS * HEAD_DIM), 1.0, 6.0, ((1, 4), (2, 2)))
    stale_keys = draw_stale_keys(jax.random.fold_in(jax.random.fold_in(key_list[14], part), 71), part)
    stale_values = bell_draw(part_keys[9], (PROMPTS, IMG, HEADS * HEAD_DIM), 1.0, 6.0, ((1, 4), (2, 2)))
    cached_residual = bell_draw(part_keys[10], (PROMPTS, IMG, D), 1.0, 6.0, ((1, 4), (2, 2)))
    patch_of = jax.random.permutation(part_keys[11], N_SEQ).astype(jnp.int32)
    refresh = draw_refresh(jax.random.fold_in(jax.random.fold_in(key_list[14], part), 71), part)
    text_len = jax.random.randint(part_keys[13], (PROMPTS,), TXT // 8, TXT + 1).astype(jnp.int32)
    return dict(image_hidden=image_hidden, modulation=modulation, qkv_weight=qkv_weight, out_weight=out_weight, q_gain=q_gain, k_gain=k_gain, text_keys=text_keys, text_values=text_values, stale_keys=stale_keys, stale_values=stale_values, cached_residual=cached_residual, patch_of=patch_of, refresh=refresh, text_len=text_len)


epsilon = 1e-06

def rotary_tables(raster, head_dim, grid_width):
    half_dim = head_dim // 2
    first_pairs = head_dim // 16
    axis_pairs = (half_dim - first_pairs) // 2
    pair_index = jnp.arange(half_dim, dtype=jnp.int32)
    pair_local = jnp.where(pair_index < first_pairs + axis_pairs, pair_index - first_pairs, pair_index - first_pairs - axis_pairs)
    exponent = -pair_local.astype(jnp.float32) / float(axis_pairs)
    frequency = jnp.where(pair_index < first_pairs, jnp.float32(0.0), jnp.power(jnp.float32(10000.0), exponent))
    row_pos = (raster // grid_width).astype(jnp.float32)
    col_pos = (raster % grid_width).astype(jnp.float32)
    position = jnp.where(pair_index[None, :] < first_pairs + axis_pairs, row_pos[:, None], col_pos[:, None])
    angles = position * frequency[None, :]
    cosine = jnp.cos(angles)
    sine = jnp.sin(angles)
    return (jnp.concatenate([cosine, cosine], axis=-1), jnp.concatenate([-sine, sine], axis=-1))

def rms_rotate(vectors, gain_vec, cos_full, sin_full):
    scaled = vectors * lax.rsqrt(lax.optimization_barrier(jnp.mean(vectors * vectors, axis=-1, keepdims=True)) + epsilon) * gain_vec
    half_dim = vectors.shape[-1] // 2
    return scaled * cos_full[:, None, :] + jnp.roll(scaled, half_dim, axis=-1) * sin_full[:, None, :]

def reference(image_hidden, modulation, qkv_weight, out_weight, q_gain, k_gain, text_keys, text_values, stale_keys, stale_values, cached_residual, patch_of, refresh, text_len):
    channels = HEADS * HEAD_DIM
    hidden_f32 = image_hidden.astype(jnp.float32)
    row_mean = lax.optimization_barrier(jnp.mean(hidden_f32, axis=-1, keepdims=True))
    centered = hidden_f32 - row_mean
    variance = lax.optimization_barrier(jnp.mean(centered * centered, axis=-1, keepdims=True))
    normed = centered * lax.rsqrt(variance + epsilon)
    modulated = (normed * (1.0 + modulation[:, 1][:, None, :]) + modulation[:, 0][:, None, :]).astype(jnp.bfloat16)
    position = jnp.arange(IMG, dtype=jnp.int32)
    owner_seat = position // IMG_DEV
    raster = patch_of[owner_seat] * IMG_DEV + position % IMG_DEV
    cos_full, sin_full = rotary_tables(raster, HEAD_DIM, GRID_W)
    refreshed = refresh[owner_seat] == 1
    score_scale = HEAD_DIM ** (-0.5)
    results = []
    for prompt in range(PROMPTS):
        projected = jnp.dot(modulated[prompt], qkv_weight.reshape(D, 3 * channels), preferred_element_type=jnp.float32)
        projected = projected.reshape(IMG, 3, HEADS, HEAD_DIM)
        fresh_q = rms_rotate(projected[:, 0], q_gain, cos_full, sin_full).astype(jnp.bfloat16)
        fresh_k = rms_rotate(projected[:, 1], k_gain, cos_full, sin_full).astype(jnp.bfloat16)
        fresh_v = projected[:, 2].astype(jnp.bfloat16)
        stale_k = stale_keys[prompt].reshape(IMG, HEADS, HEAD_DIM)
        stale_v = stale_values[prompt].reshape(IMG, HEADS, HEAD_DIM)
        text_key_rows = text_keys[prompt].reshape(TXT, HEADS, HEAD_DIM)
        text_value_rows = text_values[prompt].reshape(TXT, HEADS, HEAD_DIM)
        key_mask = jnp.concatenate([jnp.arange(TXT, dtype=jnp.int32) < text_len[prompt], jnp.ones((IMG,), jnp.bool_)])

        def attend(seq_index):
            use_fresh = refreshed | (owner_seat == seq_index)
            key_rows = jnp.where(use_fresh[:, None, None], fresh_k, stale_k)
            value_rows = jnp.where(use_fresh[:, None, None], fresh_v, stale_v)
            all_keys = jnp.concatenate([text_key_rows, key_rows], axis=0)
            all_values = jnp.concatenate([text_value_rows, value_rows], axis=0)
            queries = lax.dynamic_slice_in_dim(fresh_q, seq_index * IMG_DEV, IMG_DEV, 0)
            scores = jnp.einsum('qhd,khd->hqk', queries.astype(jnp.float32), all_keys.astype(jnp.float32)) * score_scale
            scores = jnp.where(key_mask[None, None, :], scores, -1e+30)
            row_top = lax.optimization_barrier(jnp.max(scores, axis=-1, keepdims=True))
            weights = jnp.exp(scores - row_top)
            row_sums = lax.optimization_barrier(jnp.sum(weights, axis=-1))
            probs = weights.astype(jnp.bfloat16)
            numerator = jnp.einsum('hqk,khd->qhd', probs.astype(jnp.float32), all_values.astype(jnp.float32))
            return (numerator / jnp.transpose(row_sums)[:, :, None]).astype(jnp.bfloat16)
        attended = lax.map(attend, jnp.arange(N_SEQ, dtype=jnp.int32)).reshape(IMG, channels)
        projection = jnp.dot(attended, out_weight, preferred_element_type=jnp.float32)
        combined = hidden_f32[prompt] + modulation[prompt, 2][None, :] * projection + cached_residual[prompt].astype(jnp.float32)
        results.append(combined.astype(jnp.bfloat16))
    return jnp.stack(results, axis=0)
```

```python
import functools

import jax
import jax.numpy as jnp
from jax import lax
from jax.experimental import pallas as pl
from jax.experimental.pallas import tpu as pltpu
from jax.sharding import PartitionSpec as P

GRID_W = 64
CHUNKS = 2
TILE = 512
PAIR = 256

epsilon = 1e-06
LOG2E = 1.4426950408889634


def rotary_tables(raster, head_dim, grid_width):
    half_dim = head_dim // 2
    first_pairs = head_dim // 16
    axis_pairs = (half_dim - first_pairs) // 2
    pair_index = jnp.arange(half_dim, dtype=jnp.int32)
    pair_local = jnp.where(
        pair_index < first_pairs + axis_pairs,
        pair_index - first_pairs,
        pair_index - first_pairs - axis_pairs,
    )
    exponent = -pair_local.astype(jnp.float32) / float(axis_pairs)
    frequency = jnp.where(
        pair_index < first_pairs, jnp.float32(0.0), jnp.power(jnp.float32(10000.0), exponent)
    )
    row_pos = (raster // grid_width).astype(jnp.float32)
    col_pos = (raster % grid_width).astype(jnp.float32)
    position = jnp.where(
        pair_index[None, :] < first_pairs + axis_pairs, row_pos[:, None], col_pos[:, None]
    )
    angles = position * frequency[None, :]
    cosine = jnp.cos(angles)
    sine = jnp.sin(angles)
    return (jnp.concatenate([cosine, cosine], axis=-1), jnp.concatenate([-sine, sine], axis=-1))


def rms_rotate(vectors, gain, cos_rows, sin_rows):
    mean_square = jnp.mean(vectors * vectors, axis=-1, keepdims=True)
    scaled = vectors * lax.rsqrt(mean_square + epsilon) * gain
    return scaled * cos_rows + pltpu.roll(scaled, vectors.shape[-1] // 2, 1) * sin_rows


def step_kernel(
    n_seq,
    refresh_ref,
    len_ref,
    mod_ref,
    gq_ref,
    gk_ref,
    cos_ref,
    sin_ref,
    image_ref,
    wqkv_ref,
    wout_ref,
    tk_ref,
    tv_ref,
    sk_ref,
    sv_ref,
    cached_ref,
    out_ref,
    xin,
    weights,
    wout,
    kv,
    chosen,
    queries,
    attended,
    out_send,
    out_recv,
    result,
    text,
    scores,
    modulated,
    load_sem,
    store_sem,
    img_send,
    img_recv,
    text_send,
    text_recv,
    kv_send,
    kv_recv,
    relay_send,
    part_send,
    part_recv,
):
    prompts, tok_rows, width_part = image_ref.shape
    model_width = 2 * width_part
    channels = wout.shape[0]
    head_dim = cos_ref.shape[1]
    heads = channels // head_dim
    text_rows = tk_ref.shape[1]
    total_text = text_rows * n_seq
    rows = tok_rows // CHUNKS
    n_chunks = prompts * CHUNKS
    n_tiles = width_part // TILE
    n_chips = n_seq // 2
    me = lax.axis_index("seq")
    side = lax.axis_index("head")
    core = lax.rem(me, 2)
    chip = me // 2
    other = 1 - side
    sibling = chip * 2 + (1 - core)

    def remote(src, dst, send, recv, where):
        return pltpu.make_async_remote_copy(
            src_ref=src,
            dst_ref=dst,
            send_sem=send,
            recv_sem=recv,
            device_id=where,
            device_id_type=pl.DeviceIdType.MESH,
        )

    loads = [
        pltpu.make_async_copy(image_ref, xin.at[side], load_sem.at[0]),
        pltpu.make_async_copy(wqkv_ref.at[0], weights.at[0], load_sem.at[1]),
        pltpu.make_async_copy(wqkv_ref.at[1], weights.at[1], load_sem.at[2]),
        pltpu.make_async_copy(wqkv_ref.at[2], weights.at[2], load_sem.at[3]),
        pltpu.make_async_copy(sk_ref, chosen.at[0], load_sem.at[4]),
        pltpu.make_async_copy(sv_ref, chosen.at[1], load_sem.at[5]),
        pltpu.make_async_copy(tk_ref, text.at[0, :, pl.ds(me * text_rows, text_rows)], load_sem.at[6]),
        pltpu.make_async_copy(tv_ref, text.at[1, :, pl.ds(me * text_rows, text_rows)], load_sem.at[7]),
        pltpu.make_async_copy(wout_ref, wout, load_sem.at[8]),
        pltpu.make_async_copy(cached_ref, result, load_sem.at[9]),
    ]
    for copy in loads:
        copy.start()

    barrier = pltpu.get_barrier_semaphore()
    for d in range(1, n_seq):
        peer = lax.rem(me + d, n_seq)
        pl.semaphore_signal(barrier, inc=1, device_id={"seq": peer}, device_id_type=pl.DeviceIdType.MESH)
    pl.semaphore_signal(barrier, inc=1, device_id={"head": other}, device_id_type=pl.DeviceIdType.MESH)
    pl.semaphore_wait(barrier, n_seq)

    def image_copy(c, half):
        p, r0 = c // CHUNKS, (c % CHUNKS) * rows
        return remote(
            image_ref.at[p, pl.ds(r0, rows)],
            xin.at[half, p, pl.ds(r0, rows)],
            img_send.at[c],
            img_recv.at[c],
            {"head": other},
        )

    def text_copy(i, owner, d, where):
        return remote(
            (tk_ref, tv_ref)[i],
            text.at[i, :, pl.ds(owner * text_rows, text_rows)],
            text_send.at[i, d],
            text_recv.at[i, owner],
            where,
        )

    def kv_copy(c, src, owner, send, where):
        p, r0 = c // CHUNKS, (c % CHUNKS) * rows
        return remote(
            src.at[:, p, pl.ds(r0, rows)],
            kv.at[owner, :, p, pl.ds(r0, rows)],
            send,
            kv_recv.at[owner, c],
            where,
        )

    def part_copy(p, t):
        return remote(
            out_send.at[p, t],
            out_recv.at[p, t],
            part_send.at[p, t],
            part_recv.at[p, t],
            {"head": other},
        )

    image_copy(0, side).start()
    image_copy(1, side).start()
    for d in range(1, n_seq):
        for i in range(2):
            text_copy(i, me, d, {"seq": lax.rem(me + d, n_seq)}).start()

    fresh_flag = refresh_ref[me] == 1

    def project(c):
        p, r0 = c // CHUNKS, (c % CHUNKS) * rows
        block = pl.ds(r0, rows)
        if c == 0:
            loads[0].wait()
        image_copy(c, other).wait_recv()
        image_copy(c, side).wait_send()
        if c + 2 < n_chunks:
            image_copy(c + 2, side).start()
        left = xin[0, p, block].astype(jnp.float32)
        right = xin[1, p, block].astype(jnp.float32)
        mean = (
            jnp.sum(left, axis=-1, keepdims=True) + jnp.sum(right, axis=-1, keepdims=True)
        ) / model_width
        left = left - mean
        right = right - mean
        variance = (
            jnp.sum(left * left, axis=-1, keepdims=True)
            + jnp.sum(right * right, axis=-1, keepdims=True)
        ) / model_width
        inverse = lax.rsqrt(variance + epsilon)
        for half, values in ((0, left), (1, right)):
            cols = pl.ds(half * width_part, width_part)
            modulated[:, cols] = (
                values * inverse * (1.0 + mod_ref[1, pl.ds(p, 1), cols])
                + mod_ref[0, pl.ds(p, 1), cols]
            ).astype(jnp.bfloat16)
        if c == 0:
            for copy in loads[1:6]:
                copy.wait()
        cos_rows, sin_rows = cos_ref[block, :], sin_ref[block, :]
        gain_q, gain_k = gq_ref[...], gk_ref[...]

        def pair(j, carry):
            start = pl.multiple_of(j * PAIR, PAIR)
            cols = pl.ds(start, PAIR)
            x = modulated[...]

            def rotated(index, gain):
                raw = jnp.dot(x, weights[index, :, cols], preferred_element_type=jnp.float32)
                pieces = [
                    rms_rotate(raw[:, i : i + head_dim], gain, cos_rows, sin_rows)
                    for i in range(0, PAIR, head_dim)
                ]
                return jnp.concatenate(pieces, axis=-1).astype(jnp.bfloat16)

            fresh_k = rotated(1, gain_k)
            kv[me, 0, p, block, cols] = fresh_k
            chosen[0, p, block, cols] = jnp.where(fresh_flag, fresh_k, chosen[0, p, block, cols])
            fresh_v = jnp.dot(x, weights[2, :, cols], preferred_element_type=jnp.float32).astype(
                jnp.bfloat16
            )
            kv[me, 1, p, block, cols] = fresh_v
            chosen[1, p, block, cols] = jnp.where(fresh_flag, fresh_v, chosen[1, p, block, cols])
            queries[p, block, cols] = rotated(0, gain_q)
            return carry

        lax.fori_loop(0, channels // PAIR, pair, 0)
        for d in range(1, n_chips):
            peer = lax.rem(chip + d, n_chips) * 2 + core
            kv_copy(c, chosen, me, kv_send.at[d, c], {"seq": peer}).start()
        kv_copy(c, chosen, me, kv_send.at[0, c], {"seq": sibling}).start()

    def relay(c):
        for d in range(1, n_chips):
            owner = lax.rem(chip + n_chips - d, n_chips) * 2 + core
            kv_copy(c, kv.at[owner], owner, relay_send.at[d, c], {"seq": sibling}).wait_recv()
            kv_copy(c, kv.at[owner], owner, relay_send.at[d, c], {"seq": sibling}).start()

    def arrive(c):
        for d in range(n_chips):
            owner = lax.rem(chip + n_chips - d, n_chips) * 2 + (1 - core)
            kv_copy(c, kv.at[owner], owner, relay_send.at[d, c], {"seq": sibling}).wait_recv()

    def looped(count, body, init):
        if count <= 4:
            for n in range(count):
                init = body(n, init)
            return init
        return lax.fori_loop(0, count, body, init)

    def times_transposed(a, b):
        return lax.dot_general(a, b, (((1,), (1,)), ((), ())), preferred_element_type=jnp.float32)

    factor = head_dim ** (-0.5) * LOG2E

    def attend(p):
        valid = lax.broadcasted_iota(jnp.int32, (1, total_text), 1) < len_ref[p]

        def folded(op, total, values):
            for i in range(0, values.shape[1], 128):
                total = op(total, values[:, i : i + 128])
            return total

        def one_head(h, carry):
            cols = pl.ds(pl.multiple_of(h * head_dim, head_dim), head_dim)
            q = queries[p, :, cols]
            s_text = times_transposed(q, text[0, p, :, cols])
            s_text = jnp.where(valid, s_text, -1e30)
            top = folded(jnp.maximum, jnp.full((tok_rows, 128), -1e30, jnp.float32), s_text)

            def score(n, best):
                s = times_transposed(q, kv[n, 0, p, :, cols])
                scores[n] = s
                return folded(jnp.maximum, best, s)

            top = looped(n_seq, score, top)
            top = jnp.max(top, axis=-1, keepdims=True)
            w_text = jnp.exp2((s_text - top) * factor)
            total = folded(jnp.add, jnp.zeros((tok_rows, 128), jnp.float32), w_text)
            mixed = jnp.dot(
                w_text.astype(jnp.bfloat16), text[1, p, :, cols], preferred_element_type=jnp.float32
            )

            def mix(n, state):
                total, mixed = state
                w = jnp.exp2((scores[n] - top) * factor)
                mixed = mixed + jnp.dot(
                    w.astype(jnp.bfloat16), kv[n, 1, p, :, cols], preferred_element_type=jnp.float32
                )
                return folded(jnp.add, total, w), mixed

            total, mixed = looped(n_seq, mix, (total, mixed))
            total = jnp.sum(total, axis=-1, keepdims=True)
            attended[p, :, cols] = (mixed / total).astype(jnp.bfloat16)
            return carry

        lax.fori_loop(0, heads, one_head, 0)

    def send_parts(p):
        for t in range(n_tiles):
            cols = pl.ds(pl.multiple_of(other * width_part + t * TILE, TILE), TILE)
            out_send[p, t] = jnp.dot(
                attended[p], wout[:, cols], preferred_element_type=jnp.float32
            ).astype(jnp.bfloat16)
            part_copy(p, t).start()

    def store(p, t):
        here = pl.ds(t * TILE, TILE)
        return pltpu.make_async_copy(
            result.at[p, :, here], out_ref.at[p, :, here], store_sem.at[p, t]
        )

    def finish(p):
        for t in range(n_tiles):
            cols = pl.ds(pl.multiple_of(side * width_part + t * TILE, TILE), TILE)
            here = pl.ds(t * TILE, TILE)
            own = jnp.dot(attended[p], wout[:, cols], preferred_element_type=jnp.float32)
            part_copy(p, t).wait_recv()
            gate = mod_ref[2, pl.ds(p, 1), cols]
            result[p, :, here] = (
                xin[side, p, :, here].astype(jnp.float32)
                + gate * (own + out_recv[p, t].astype(jnp.float32))
                + result[p, :, here].astype(jnp.float32)
            ).astype(jnp.bfloat16)
            store(p, t).start()

    project(0)
    for c in range(1, n_chunks):
        project(c)
        relay(c - 1)
        if c == CHUNKS:
            for copy in loads[6:]:
                copy.wait()
            for d in range(1, n_seq):
                for i in range(2):
                    text_copy(i, lax.rem(me + d, n_seq), d, {"seq": sibling}).wait_recv()
        if c >= CHUNKS and c % CHUNKS == 0:
            p = c // CHUNKS - 1
            for k in range(p * CHUNKS, (p + 1) * CHUNKS):
                arrive(k)
            attend(p)
            send_parts(p)
    relay(n_chunks - 1)
    for k in range(n_chunks - CHUNKS, n_chunks):
        arrive(k)
    attend(prompts - 1)
    send_parts(prompts - 1)
    for p in range(prompts):
        finish(p)

    for p in range(prompts):
        for t in range(n_tiles):
            part_copy(p, t).wait_send()
            store(p, t).wait()
    for c in range(n_chunks):
        for d in range(n_chips):
            kv_copy(c, chosen, me, kv_send.at[d, c], {"seq": sibling}).wait_send()
        for d in range(1, n_chips):
            kv_copy(c, chosen, me, relay_send.at[d, c], {"seq": sibling}).wait_send()
    for d in range(1, n_seq):
        for i in range(2):
            text_copy(i, me, d, {"seq": sibling}).wait_send()


def per_device(
    n_seq,
    image_hidden,
    modulation,
    qkv_weight,
    out_weight,
    q_gain,
    k_gain,
    text_keys,
    text_values,
    stale_keys,
    stale_values,
    cached_residual,
    patch_of,
    refresh,
    text_len,
):
    prompts, tok_rows, width_part = image_hidden.shape
    head_dim = q_gain.shape[0]
    channels, model_width = out_weight.shape
    text_rows = text_keys.shape[1]
    seq_seat = lax.axis_index("seq")
    own_band = lax.dynamic_index_in_dim(patch_of, seq_seat, 0, keepdims=False)
    raster = own_band * tok_rows + jnp.arange(tok_rows, dtype=jnp.int32)
    cos_full, sin_full = rotary_tables(raster, head_dim, GRID_W)
    n_chunks = prompts * CHUNKS
    n_tiles = width_part // TILE
    n_chips = n_seq // 2
    bf16 = jnp.bfloat16
    dma = pltpu.SemaphoreType.DMA
    smem = pl.BlockSpec(memory_space=pltpu.SMEM)
    vmem = pl.BlockSpec(memory_space=pltpu.VMEM)
    anywhere = pl.BlockSpec(memory_space=pl.ANY)
    return pl.pallas_call(
        functools.partial(step_kernel, n_seq),
        out_shape=jax.ShapeDtypeStruct(image_hidden.shape, bf16),
        in_specs=[smem] * 2 + [vmem] * 5 + [anywhere] * 8,
        out_specs=anywhere,
        scratch_shapes=[
            pltpu.VMEM((2, prompts, tok_rows, width_part), bf16),
            pltpu.VMEM((3, model_width, channels), bf16),
            pltpu.VMEM((channels, model_width), bf16),
            pltpu.VMEM((n_seq, 2, prompts, tok_rows, channels), bf16),
            pltpu.VMEM((2, prompts, tok_rows, channels), bf16),
            pltpu.VMEM((prompts, tok_rows, channels), bf16),
            pltpu.VMEM((prompts, tok_rows, channels), bf16),
            pltpu.VMEM((prompts, n_tiles, tok_rows, TILE), bf16),
            pltpu.VMEM((prompts, n_tiles, tok_rows, TILE), bf16),
            pltpu.VMEM((prompts, tok_rows, width_part), bf16),
            pltpu.VMEM((2, prompts, text_rows * n_seq, channels), bf16),
            pltpu.VMEM((n_seq, tok_rows, tok_rows), jnp.float32),
            pltpu.VMEM((tok_rows // CHUNKS, model_width), bf16),
            dma((10,)),
            dma((prompts, n_tiles)),
            dma((n_chunks,)),
            dma((n_chunks,)),
            dma((2, n_seq)),
            dma((2, n_seq)),
            dma((n_chips, n_chunks)),
            dma((n_seq, n_chunks)),
            dma((n_chips, n_chunks)),
            dma((prompts, n_tiles)),
            dma((prompts, n_tiles)),
        ],
        compiler_params=pltpu.CompilerParams(
            collective_id=0, has_side_effects=True, vmem_limit_bytes=67043328
        ),
        name="joint_step",
    )(
        refresh,
        text_len,
        jnp.transpose(modulation, (1, 0, 2)),
        q_gain[None],
        k_gain[None],
        cos_full,
        sin_full,
        image_hidden,
        jnp.transpose(qkv_weight, (1, 0, 2)),
        out_weight,
        text_keys,
        text_values,
        stale_keys,
        stale_values,
        cached_residual,
    )


def solution(mesh):
    in_specs = (
        P("batch", "seq", "head"),
        P("batch", None, None),
        P(None, None, "head"),
        P("head", None),
        P(),
        P(),
        P("batch", "seq", "head"),
        P("batch", "seq", "head"),
        P("batch", "seq", "head"),
        P("batch", "seq", "head"),
        P("batch", "seq", "head"),
        P("batch"),
        P("batch"),
        P("batch"),
    )
    out_specs = P("batch", "seq", "head")
    return jax.shard_map(
        functools.partial(per_device, mesh.shape["seq"]),
        mesh=mesh,
        in_specs=in_specs,
        out_specs=out_specs,
        check_vma=False,
    )
```

```python
import functools

import jax
import jax.numpy as jnp
from jax import lax
from jax.experimental import pallas as pl
from jax.experimental.pallas import tpu as pltpu
from jax.sharding import PartitionSpec as P

GRID_W = 64
FIRST = (4, 4, 2)
LAST = (2, 4, 4)
MIDDLE = (2, 2)
LAG = 2
W_SPREAD = 0
TILE = 512
PAIR = 256

epsilon = 1e-06
LOG2E = 1.4426950408889634


def rotary_tables(raster, head_dim, grid_width):
    half_dim = head_dim // 2
    first_pairs = head_dim // 16
    axis_pairs = (half_dim - first_pairs) // 2
    lane = jnp.arange(head_dim, dtype=jnp.int32)
    pair_index = lane % half_dim
    pair_local = jnp.where(
        pair_index < first_pairs + axis_pairs,
        pair_index - first_pairs,
        pair_index - first_pairs - axis_pairs,
    )
    exponent = -pair_local.astype(jnp.float32) / float(axis_pairs)
    frequency = jnp.where(
        pair_index < first_pairs, jnp.float32(0.0), jnp.power(jnp.float32(10000.0), exponent)
    )
    row_pos = (raster // grid_width).astype(jnp.float32)
    col_pos = (raster % grid_width).astype(jnp.float32)
    position = jnp.where(
        pair_index[None, :] < first_pairs + axis_pairs, row_pos[:, None], col_pos[:, None]
    )
    angles = position * frequency[None, :]
    sign = jnp.where(lane < half_dim, -1.0, 1.0)
    return jnp.cos(angles), jnp.sin(angles) * sign[None, :]


def chunk_table(prompts, tok_rows):
    table = []
    for p in range(prompts):
        r0 = 0
        for cut in FIRST if p == 0 else LAST if p == prompts - 1 else MIDDLE:
            table.append((p, r0, tok_rows // cut))
            r0 += tok_rows // cut
    return table


def rms_rotate(vectors, gain, cos_rows, sin_rows):
    mean_square = jnp.mean(vectors * vectors, axis=-1, keepdims=True)
    scaled = vectors * lax.rsqrt(mean_square + epsilon) * gain
    return scaled * cos_rows + pltpu.roll(scaled, vectors.shape[-1] // 2, 1) * sin_rows


def step_kernel(
    n_seq,
    n_batch,
    refresh_ref,
    len_ref,
    mod_ref,
    gq_ref,
    gk_ref,
    cos_ref,
    sin_ref,
    image_ref,
    wqkv_ref,
    wout_ref,
    tk_ref,
    tv_ref,
    sk_ref,
    sv_ref,
    cached_ref,
    out_ref,
    xin,
    weights,
    wfull,
    kv,
    chosen,
    queries,
    attended,
    partial,
    result,
    text,
    score_slots,
    modulated,
    load_sem,
    store_sem,
    img_send,
    img_recv,
    text_send,
    text_recv,
    kv_send,
    kv_recv,
    relay_send,
    part_send,
    part_recv,
    w_send,
    w_recv,
    w_spread,
):
    prompts, tok_rows, width_part = image_ref.shape
    model_width = 2 * width_part
    channels = wout_ref.shape[0]
    head_dim = cos_ref.shape[1]
    heads = channels // head_dim
    text_rows = tk_ref.shape[1]
    total_text = text_rows * n_seq
    table = chunk_table(prompts, tok_rows)
    n_chunks = len(table)
    n_tiles = width_part // TILE
    n_chips = n_seq // 2
    n_pairs = channels // PAIR
    w_rows = channels // (2 * n_batch)
    part = lax.axis_index("batch")
    me = lax.axis_index("seq")
    side = lax.axis_index("head")
    core = lax.rem(me, 2)
    chip = me // 2
    other = 1 - side
    sibling = chip * 2 + (1 - core)

    def remote(src, dst, send, recv, where):
        return pltpu.make_async_remote_copy(
            src_ref=src,
            dst_ref=dst,
            send_sem=send,
            recv_sem=recv,
            device_id=where,
            device_id_type=pl.DeviceIdType.MESH,
        )

    loads = [
        pltpu.make_async_copy(image_ref, xin.at[side], load_sem.at[0]),
        pltpu.make_async_copy(wqkv_ref.at[0], weights.at[0], load_sem.at[1]),
        pltpu.make_async_copy(wqkv_ref.at[1], weights.at[1], load_sem.at[2]),
        pltpu.make_async_copy(wqkv_ref.at[2], weights.at[2], load_sem.at[3]),
        pltpu.make_async_copy(sk_ref, chosen.at[0], load_sem.at[4]),
        pltpu.make_async_copy(sv_ref, chosen.at[1], load_sem.at[5]),
        pltpu.make_async_copy(tk_ref, text.at[0, :, pl.ds(me * text_rows, text_rows)], load_sem.at[6]),
        pltpu.make_async_copy(tv_ref, text.at[1, :, pl.ds(me * text_rows, text_rows)], load_sem.at[7]),
        pltpu.make_async_copy(
            wout_ref.at[:, pl.ds(pl.multiple_of(side * width_part, width_part), width_part)],
            wfull.at[side],
            load_sem.at[8],
        ),
        pltpu.make_async_copy(cached_ref, result, load_sem.at[9]),
    ]
    for copy in loads:
        copy.start()

    barrier = pltpu.get_barrier_semaphore()
    for d in range(1, n_seq):
        peer = lax.rem(me + d, n_seq)
        pl.semaphore_signal(barrier, inc=1, device_id={"seq": peer}, device_id_type=pl.DeviceIdType.MESH)
    pl.semaphore_signal(barrier, inc=1, device_id={"head": other}, device_id_type=pl.DeviceIdType.MESH)
    for d in range(1, n_batch):
        peer = lax.rem(part + d, n_batch)
        pl.semaphore_signal(barrier, inc=1, device_id={"batch": peer}, device_id_type=pl.DeviceIdType.MESH)
    pl.semaphore_wait(barrier, n_seq + n_batch - 1)

    def image_copy(c, half):
        p, r0, rows = table[c]
        return remote(
            image_ref.at[p, pl.ds(r0, rows)],
            xin.at[half, p, pl.ds(r0, rows)],
            img_send.at[c],
            img_recv.at[c],
            {"head": other},
        )

    def text_copy(i, owner, d, where):
        return remote(
            (tk_ref, tv_ref)[i],
            text.at[i, :, pl.ds(owner * text_rows, text_rows)],
            text_send.at[i, d],
            text_recv.at[i, owner],
            where,
        )

    def kv_copy(c, src, owner, send, where):
        p, r0, rows = table[c]
        return remote(
            src.at[:, p, pl.ds(r0, rows)],
            kv.at[owner, :, p, pl.ds(r0, rows)],
            send,
            kv_recv.at[owner, c],
            where,
        )

    def part_copy(p, j, half):
        cols = pl.ds(j * PAIR if isinstance(j, int) else pl.multiple_of(j * PAIR, PAIR), PAIR)
        return remote(
            attended.at[half, p, :, cols],
            attended.at[half, p, :, cols],
            part_send.at[p, j],
            part_recv.at[p, j],
            {"head": other},
        )

    def w_block(owner, which):
        return wfull.at[other, pl.ds((owner * 2 + which) * w_rows, w_rows)]

    def w_cross(half):
        block = pl.ds((part * 2 + core) * w_rows, w_rows)
        cols = pl.ds(pl.multiple_of(other * width_part, width_part), width_part)
        return remote(
            wout_ref.at[block, cols],
            wfull.at[half, block],
            w_send.at[0],
            w_recv.at[part, core],
            {"head": other},
        )

    def w_along(owner, d, where):
        return remote(
            w_block(owner, core), w_block(owner, core), w_send.at[d], w_recv.at[owner, core], where
        )

    def w_to_sibling(owner, which, d):
        return remote(
            w_block(owner, which),
            w_block(owner, which),
            w_spread.at[d],
            w_recv.at[owner, which],
            {"seq": sibling},
        )

    def spread_weights():
        w_cross(other).wait_recv()
        for d in range(1, n_batch):
            w_along(part, d, {"batch": lax.rem(part + d, n_batch)}).start()
        w_to_sibling(part, core, 0).start()

    def relay_weights():
        for d in range(1, n_batch):
            owner = lax.rem(part + n_batch - d, n_batch)
            w_along(owner, d, {"batch": owner}).wait_recv()
            w_to_sibling(owner, core, d).start()

    def weights_here():
        for d in range(n_batch):
            w_to_sibling(lax.rem(part + d, n_batch), 1 - core, d).wait_recv()

    w_cross(side).start()
    image_copy(0, side).start()
    image_copy(1, side).start()
    for d in range(1, n_seq):
        for i in range(2):
            text_copy(i, me, d, {"seq": lax.rem(me + d, n_seq)}).start()

    fresh_flag = refresh_ref[me] == 1

    def project(c):
        p, r0, rows = table[c]
        block = pl.ds(r0, rows)
        if c == 0:
            loads[0].wait()
        image_copy(c, other).wait_recv()
        image_copy(c, side).wait_send()
        if c + 2 < n_chunks:
            image_copy(c + 2, side).start()
        left = xin[0, p, block].astype(jnp.float32)
        right = xin[1, p, block].astype(jnp.float32)
        mean = (
            jnp.sum(left, axis=-1, keepdims=True) + jnp.sum(right, axis=-1, keepdims=True)
        ) / model_width
        left = left - mean
        right = right - mean
        variance = (
            jnp.sum(left * left, axis=-1, keepdims=True)
            + jnp.sum(right * right, axis=-1, keepdims=True)
        ) / model_width
        inverse = lax.rsqrt(variance + epsilon)
        for half, values in ((0, left), (1, right)):
            cols = pl.ds(half * width_part, width_part)
            modulated[pl.ds(0, rows), cols] = (
                values * inverse * (1.0 + mod_ref[1, pl.ds(p, 1), cols])
                + mod_ref[0, pl.ds(p, 1), cols]
            ).astype(jnp.bfloat16)
        if c == 0:
            for copy in loads[1:6]:
                copy.wait()
        cos_rows, sin_rows = cos_ref[block, :], sin_ref[block, :]
        gain_q, gain_k = gq_ref[...], gk_ref[...]

        def pair(j, carry):
            start = pl.multiple_of(j * PAIR, PAIR)
            cols = pl.ds(start, PAIR)
            x = modulated[pl.ds(0, rows)]

            def rotated(index, gain):
                raw = jnp.dot(x, weights[index, :, cols], preferred_element_type=jnp.float32)
                pieces = [
                    rms_rotate(raw[:, i : i + head_dim], gain, cos_rows, sin_rows)
                    for i in range(0, PAIR, head_dim)
                ]
                return jnp.concatenate(pieces, axis=-1).astype(jnp.bfloat16)

            fresh_k = rotated(1, gain_k)
            kv[me, 0, p, block, cols] = fresh_k
            chosen[0, p, block, cols] = jnp.where(fresh_flag, fresh_k, chosen[0, p, block, cols])
            fresh_v = jnp.dot(x, weights[2, :, cols], preferred_element_type=jnp.float32).astype(
                jnp.bfloat16
            )
            kv[me, 1, p, block, cols] = fresh_v
            chosen[1, p, block, cols] = jnp.where(fresh_flag, fresh_v, chosen[1, p, block, cols])
            queries[p, block, cols] = rotated(0, gain_q)
            return carry

        lax.fori_loop(0, channels // PAIR, pair, 0)
        for d in range(1, n_chips):
            peer = lax.rem(chip + d, n_chips) * 2 + core
            kv_copy(c, chosen, me, kv_send.at[d, c], {"seq": peer}).start()
        kv_copy(c, chosen, me, kv_send.at[0, c], {"seq": sibling}).start()

    def relay(c):
        for d in range(1, n_chips):
            owner = lax.rem(chip + n_chips - d, n_chips) * 2 + core
            kv_copy(c, kv.at[owner], owner, relay_send.at[d, c], {"seq": sibling}).wait_recv()
            kv_copy(c, kv.at[owner], owner, relay_send.at[d, c], {"seq": sibling}).start()

    def arrive(c):
        for d in range(n_chips):
            owner = lax.rem(chip + n_chips - d, n_chips) * 2 + (1 - core)
            kv_copy(c, kv.at[owner], owner, relay_send.at[d, c], {"seq": sibling}).wait_recv()

    def looped(count, body, init):
        if count <= 4:
            for n in range(count):
                init = body(n, init)
            return init
        return lax.fori_loop(0, count, body, init)

    def times_transposed(a, b):
        return lax.dot_general(a, b, (((1,), (1,)), ((), ())), preferred_element_type=jnp.float32)

    factor = head_dim ** (-0.5) * LOG2E

    def attend(p):
        valid = lax.broadcasted_iota(jnp.int32, (1, total_text), 1) < len_ref[p]

        def folded(op, total, values):
            for i in range(0, values.shape[1], 128):
                total = op(total, values[:, i : i + 128])
            return total

        def one_head(h, slot):
            scores = score_slots.at[slot]
            cols = pl.ds(pl.multiple_of(h * head_dim, head_dim), head_dim)
            q = queries[p, :, cols]
            s_text = times_transposed(q, text[0, p, :, cols])
            s_text = jnp.where(valid, s_text, -1e30)
            top = folded(jnp.maximum, jnp.full((tok_rows, 128), -1e30, jnp.float32), s_text)

            def score(n, best):
                s = times_transposed(q, kv[n, 0, p, :, cols])
                scores[n] = s
                return folded(jnp.maximum, best, s)

            top = looped(n_seq, score, top)
            top = jnp.max(top, axis=-1, keepdims=True)
            w_text = jnp.exp2((s_text - top) * factor)
            total = folded(jnp.add, jnp.zeros((tok_rows, 128), jnp.float32), w_text)
            mixed = jnp.dot(
                w_text.astype(jnp.bfloat16), text[1, p, :, cols], preferred_element_type=jnp.float32
            )

            def mix(n, state):
                total, mixed = state
                w = jnp.exp2((scores[n] - top) * factor)
                mixed = mixed + jnp.dot(
                    w.astype(jnp.bfloat16), kv[n, 1, p, :, cols], preferred_element_type=jnp.float32
                )
                return folded(jnp.add, total, w), mixed

            total, mixed = looped(n_seq, mix, (total, mixed))
            total = jnp.sum(total, axis=-1, keepdims=True)
            attended[side, p, :, cols] = (mixed / total).astype(jnp.bfloat16)

        def head_pair(j, carry):
            for i in range(PAIR // head_dim):
                one_head(j * (PAIR // head_dim) + i, i % score_slots.shape[0])
            part_copy(p, j, side).start()
            return carry

        lax.fori_loop(0, n_pairs, head_pair, 0)

    def store(p, t):
        here = pl.ds(t * TILE, TILE)
        return pltpu.make_async_copy(
            result.at[p, :, here], out_ref.at[p, :, here], store_sem.at[p, t]
        )

    def finish(p):
        early = (n_pairs - 1) * PAIR

        def accumulate(half, first, last, t):
            return jnp.dot(
                attended[half, p, :, first:last],
                wfull[half, first:last, t * TILE : (t + 1) * TILE],
                preferred_element_type=jnp.float32,
            )

        for t in range(n_tiles):
            partial[t] = accumulate(side, 0, channels, t)
        for j in range(n_pairs - 1):
            part_copy(p, j, other).wait_recv()
        for t in range(n_tiles):
            partial[t] += accumulate(other, 0, early, t)
        part_copy(p, n_pairs - 1, other).wait_recv()
        for t in range(n_tiles):
            cols = pl.ds(pl.multiple_of(side * width_part + t * TILE, TILE), TILE)
            here = pl.ds(t * TILE, TILE)
            whole = partial[t] + accumulate(other, early, channels, t)
            gate = mod_ref[2, pl.ds(p, 1), cols]
            result[p, :, here] = (
                xin[side, p, :, here].astype(jnp.float32)
                + gate * whole
                + result[p, :, here].astype(jnp.float32)
            ).astype(jnp.bfloat16)
            store(p, t).start()

    def attend_all(p):
        for k in range(n_chunks):
            if table[k][0] == p:
                arrive(k)
        attend(p)

    for c in range(n_chunks):
        project(c)
        if c == W_SPREAD:
            spread_weights()
        if c >= LAG:
            relay(c - LAG)
    for copy in loads[6:]:
        copy.wait()
    for d in range(1, n_seq):
        for i in range(2):
            text_copy(i, lax.rem(me + d, n_seq), d, {"seq": sibling}).wait_recv()
    for p in range(prompts - 1):
        attend_all(p)
    for c in range(n_chunks - LAG, n_chunks):
        relay(c)
    attend_all(prompts - 1)
    relay_weights()
    weights_here()
    for p in range(prompts):
        finish(p)

    for p in range(prompts):
        for j in range(n_pairs):
            part_copy(p, j, side).wait_send()
        for t in range(n_tiles):
            store(p, t).wait()
    w_cross(side).wait_send()
    for d in range(1, n_batch):
        w_along(part, d, {"batch": lax.rem(part + d, n_batch)}).wait_send()
    for d in range(n_batch):
        w_to_sibling(lax.rem(part + n_batch - d, n_batch), core, d).wait_send()
    for c in range(n_chunks):
        for d in range(n_chips):
            kv_copy(c, chosen, me, kv_send.at[d, c], {"seq": sibling}).wait_send()
        for d in range(1, n_chips):
            kv_copy(c, chosen, me, relay_send.at[d, c], {"seq": sibling}).wait_send()
    for d in range(1, n_seq):
        for i in range(2):
            text_copy(i, me, d, {"seq": sibling}).wait_send()


def per_device(
    n_seq,
    n_batch,
    image_hidden,
    modulation,
    qkv_weight,
    out_weight,
    q_gain,
    k_gain,
    text_keys,
    text_values,
    stale_keys,
    stale_values,
    cached_residual,
    patch_of,
    refresh,
    text_len,
):
    prompts, tok_rows, width_part = image_hidden.shape
    head_dim = q_gain.shape[0]
    channels, model_width = out_weight.shape
    text_rows = text_keys.shape[1]
    seq_seat = lax.axis_index("seq")
    seats = jnp.arange(n_seq, dtype=jnp.int32)
    own_band = jnp.sum(jnp.where(seats == seq_seat, patch_of, 0))
    raster = own_band * tok_rows + jnp.arange(tok_rows, dtype=jnp.int32)
    cos_full, sin_full = rotary_tables(raster, head_dim, GRID_W)
    n_chunks = len(chunk_table(prompts, tok_rows))
    n_tiles = width_part // TILE
    n_chips = n_seq // 2
    bf16 = jnp.bfloat16
    dma = pltpu.SemaphoreType.DMA
    smem = pl.BlockSpec(memory_space=pltpu.SMEM)
    vmem = pl.BlockSpec(memory_space=pltpu.VMEM)
    anywhere = pl.BlockSpec(memory_space=pl.ANY)
    return pl.pallas_call(
        functools.partial(step_kernel, n_seq, n_batch),
        out_shape=jax.ShapeDtypeStruct(image_hidden.shape, bf16),
        in_specs=[smem] * 2 + [vmem] * 5 + [anywhere] * 8,
        out_specs=anywhere,
        scratch_shapes=[
            pltpu.VMEM((2, prompts, tok_rows, width_part), bf16),
            pltpu.VMEM((3, model_width, channels), bf16),
            pltpu.VMEM((2, channels, width_part), bf16),
            pltpu.VMEM((n_seq, 2, prompts, tok_rows, channels), bf16),
            pltpu.VMEM((2, prompts, tok_rows, channels), bf16),
            pltpu.VMEM((prompts, tok_rows, channels), bf16),
            pltpu.VMEM((2, prompts, tok_rows, channels), bf16),
            pltpu.VMEM((n_tiles, tok_rows, TILE), jnp.float32),
            pltpu.VMEM((prompts, tok_rows, width_part), bf16),
            pltpu.VMEM((2, prompts, text_rows * n_seq, channels), bf16),
            pltpu.VMEM((2 if n_seq <= 4 else 1, n_seq, tok_rows, tok_rows), jnp.float32),
            pltpu.VMEM((tok_rows // 2, model_width), bf16),
            dma((10,)),
            dma((prompts, n_tiles)),
            dma((n_chunks,)),
            dma((n_chunks,)),
            dma((2, n_seq)),
            dma((2, n_seq)),
            dma((n_chips, n_chunks)),
            dma((n_seq, n_chunks)),
            dma((n_chips, n_chunks)),
            dma((prompts, channels // PAIR)),
            dma((prompts, channels // PAIR)),
            dma((n_batch,)),
            dma((n_batch, 2)),
            dma((n_batch,)),
        ],
        compiler_params=pltpu.CompilerParams(
            collective_id=0, has_side_effects=True, vmem_limit_bytes=67043328
        ),
        name="joint_step",
    )(
        refresh,
        text_len,
        jnp.transpose(modulation, (1, 0, 2)),
        q_gain[None],
        k_gain[None],
        cos_full,
        sin_full,
        image_hidden,
        jnp.transpose(qkv_weight, (1, 0, 2)),
        out_weight,
        text_keys,
        text_values,
        stale_keys,
        stale_values,
        cached_residual,
    )


def solution(mesh):
    in_specs = (
        P("batch", "seq", "head"),
        P("batch", None, None),
        P(None, None, "head"),
        P("head", None),
        P(),
        P(),
        P("batch", "seq", "head"),
        P("batch", "seq", "head"),
        P("batch", "seq", "head"),
        P("batch", "seq", "head"),
        P("batch", "seq", "head"),
        P("batch"),
        P("batch"),
        P("batch"),
    )
    out_specs = P("batch", "seq", "head")
    return jax.shard_map(
        functools.partial(per_device, mesh.shape["seq"], mesh.shape["batch"]),
        mesh=mesh,
        in_specs=in_specs,
        out_specs=out_specs,
        check_vma=False,
    )
```
